32 devices in a mesh: blk: 8 (over z, x), order: 4 (over y, core).
Axes of the slice: x: 2, y: 2, z: 4, core: 2. Of those that a mesh axis runs over, the one named last changes fastest.
Arguments:
- field: float32 [16, 512, 4096], P(None, 'blk', 'order'), may hold values from -6 to 6
- ocean_mask: int32 [512, 4096], P('blk', 'order'), may hold values from 0 to 1, as said below
- plan: int32 [512], replicated, may hold values from 0 to 384, as said below
- legendre: bfloat16 [384, 1024, 1024], P('blk', 'order'), may hold values from -0.4375 to 0.4375
Outputs:
- coefficients: float32 [1024, 16, 2, 1024], P('blk', None, None, 'order')
The draws below stay inside these ranges and needn't reach their ends.
Inputs may be any that keep to these rules, and one draw needn't show every extreme that they name: `ocean_mask`: exactly 128 cycles are all land, at the ends of the cycle order; every other cycle has an ocean point. plan is 384 exactly at the cycles that are all land, and names every slot below 384 once at the other cycles; slot p belongs to index p // 48 of blk; the cycles of one index of blk name at most 8 slots of one index, and in every draw some index of blk names exactly 8 slots of some index.
All inputs are finite; a program needn't handle non-finite values.
Results may differ from the reference program's by a relative error of at most 0.0029.
Values may be sent and summed in bfloat16 or wider, within the bound.
A program may use at most 128 MiB of HBM per device.

```python
import jax
import jax.numpy as jnp
from jax import lax

NLON = 4096
M = 1024
L = 1024
FIELDS = 16
CYCLES = 512
SLOT_DEV = 48
SLOTS = 384
N_BLK = 8
N_ORDER = 4


def wet_cycles(key):
    folded = jax.random.fold_in(key, 11)
    dry_count = CYCLES - SLOTS
    south = jax.random.randint(folded, (), 0, dry_count + 1)
    cycles = jnp.arange(CYCLES, dtype=jnp.int32)
    inside = (cycles >= south) & (cycles < CYCLES - dry_count + south)
    return inside.astype(jnp.int32)


def draw_plan(key, part):
    wet = wet_cycles(key)
    counted = jnp.cumsum(wet).astype(jnp.int32) - 1
    owner_slot = counted % N_BLK * SLOT_DEV + counted // N_BLK
    return jnp.where(wet == 1, owner_slot, SLOTS).astype(jnp.int32)


def draw_ocean_mask(key, part):
    wet = wet_cycles(key)
    levels = jax.random.randint(jax.random.fold_in(key, 12), (CYCLES, NLON), 0, 10)
    cycles = jnp.arange(CYCLES, dtype=jnp.int32)[:, None]
    longitudes = jnp.arange(NLON, dtype=jnp.int32)[None, :]
    forced = longitudes == cycles * 37 % NLON
    ocean = ((levels < 7) | forced) & (wet[:, None] == 1)
    return ocean.astype(jnp.int32)


def strengthened(drawn, own_key, source, target, shards_of, factor):
    owner, partner = [(jnp.arange(drawn.shape[dim]) // (drawn.shape[dim] // shards_of)).reshape([-1 if axis == dim else 1 for axis in range(drawn.ndim)]) for dim in (source, target)]
    chosen = jax.random.permutation(own_key, shards_of)[partner]
    strong = (owner == chosen) | (owner == (partner + shards_of // 2) % shards_of)
    return jnp.where(strong, factor * drawn, drawn)


def block_scale(stream_key, shape, cuts, least, high):
    gain = 1.0
    for position, blocks in cuts:
        steps = jax.random.uniform(jax.random.fold_in(jax.random.fold_in(stream_key, 6), position), (blocks,), jnp.float32, least / len(cuts), high / len(cuts))
        gain = gain * jnp.repeat(jnp.exp(steps), shape[position] // blocks).reshape((-1,) + (1,) * (len(shape) - 1 - position))
    return gain


def noise(key, shape, deviation, bound, shards=(), kind=jnp.bfloat16):
    result = deviation * jax.random.normal(key, shape, jnp.float32)
    if shards:
        result = result * block_scale(key, shape, shards, -0.22, 0.18)
    return jnp.clip(result, -bound, bound).astype(kind)


def gaussian_with(own_key, shape, scale, bound, shards, heavy, kind=jnp.bfloat16):
    drawn = scale * jax.random.normal(own_key, shape, jnp.float32)
    if shards:
        drawn = drawn * block_scale(own_key, shape, shards, -0.22, 0.18)
    return jnp.clip(strengthened(drawn, jax.random.fold_in(own_key, 3), *heavy), -bound, bound).astype(kind)


def setup_inputs(seed: int = 0) -> dict:
    key_list = jax.random.split(jax.random.key(seed), 5)
    field = noise(key_list[0], (FIELDS, CYCLES, NLON), 1.0, 6.0, ((1, 8), (2, 4)), jnp.float32)
    ocean_mask = draw_ocean_mask(jax.random.fold_in(key_list[4], 71), 0)
    plan = draw_plan(jax.random.fold_in(key_list[4], 71), 0)
    legendre = gaussian_with(key_list[3], (SLOTS, M, L), SLOTS ** -0.5, 0.4375, ((0, 8), (1, 4)), (0, 2, 8, 2.0))
    return dict(field=field, ocean_mask=ocean_mask, plan=plan, legendre=legendre)


def reference(field, ocean_mask, plan, legendre):
    masked = field * ocean_mask.astype(jnp.float32)[None]
    holder = jnp.zeros((FIELDS, SLOTS + 1, NLON), jnp.float32)
    packed = holder.at[:, plan.astype(jnp.int32), :].set(masked)[:, :SLOTS]
    transform = jnp.fft.rfft(packed, axis=2)[:, :, :M] / jnp.sqrt(jnp.float32(NLON))
    spectrum = jnp.stack([jnp.real(transform), jnp.imag(transform)], axis=2).astype(jnp.float32).astype(jnp.bfloat16)
    width = M // N_ORDER

    def one_block(block_index):
        first = (block_index * width).astype(jnp.int32)
        table = lax.dynamic_slice_in_dim(legendre, first, width, 1).astype(jnp.float32)
        values = lax.dynamic_slice_in_dim(spectrum, first, width, 3).astype(jnp.float32)
        return jnp.einsum('pml,fpcm->lfcm', table, values)
    blocks = lax.map(one_block, jnp.arange(N_ORDER, dtype=jnp.int32))
    moved = jnp.moveaxis(blocks, 0, 3)
    return moved.reshape(L, FIELDS, 2, M)
```

```python
import math

import jax
import jax.numpy as jnp
from jax import lax
from jax.sharding import PartitionSpec as P

NLON = 4096
M = 1024


def twiddle(first, count):
    longitudes = first + jnp.arange(count, dtype=jnp.int32)
    orders = jnp.arange(M, dtype=jnp.int32)
    product = longitudes[:, None] * orders[None, :] % NLON
    angle = product.astype(jnp.float32) * (2.0 * math.pi / NLON)
    scale = 1.0 / math.sqrt(NLON)
    return jnp.stack([jnp.cos(angle) * scale, -jnp.sin(angle) * scale], axis=1)


def transform(values, table):
    return jnp.einsum("frn,ncm->frcm", values, table, precision=lax.Precision.HIGHEST)


def pack_cycles(masked, plan, slot_dev):
    n_blk = lax.axis_size("blk")
    own_index = lax.axis_index("blk")
    cycle_dev = masked.shape[1]
    cap = (cycle_dev + n_blk - 1) // n_blk
    grid = plan.reshape(n_blk, cycle_dev)
    owner = grid // slot_dev
    positions = jnp.arange(cycle_dev, dtype=jnp.int32)
    earlier = positions[None, :] < positions[:, None]
    same_owner = owner[:, :, None] == owner[:, None, :]
    rank = jnp.sum(same_owner & earlier[None], axis=2, dtype=jnp.int32)
    send_pos = owner * cap + rank
    local_pos = lax.dynamic_index_in_dim(send_pos, own_index, 0, keepdims=False)
    buffer_ids = jnp.arange(n_blk * cap, dtype=jnp.int32)
    send_onehot = (buffer_ids[:, None] == local_pos[None, :]).astype(jnp.float32)
    outgoing = jnp.einsum("qr,frn->fqn", send_onehot, masked, precision=lax.Precision.HIGHEST)
    arrived = lax.all_to_all(outgoing, "blk", split_axis=1, concat_axis=1, tiled=True)
    source_pos = (jnp.arange(n_blk, dtype=jnp.int32)[:, None] * cap + rank).reshape(-1)
    mine = (owner == own_index).reshape(-1)
    slot_local = (grid % slot_dev).reshape(-1)
    slot_ids = jnp.arange(slot_dev, dtype=jnp.int32)
    slot_onehot = ((slot_local[None, :] == slot_ids[:, None]) & mine[None, :]).astype(jnp.float32)
    source_onehot = (source_pos[:, None] == buffer_ids[None, :]).astype(jnp.float32)
    receive_map = jnp.dot(slot_onehot, source_onehot, precision=lax.Precision.HIGHEST)
    return jnp.einsum("pq,fqn->fpn", receive_map, arrived, precision=lax.Precision.HIGHEST)


def degree_sums(legendre, spectrum):
    n_blk = lax.axis_size("blk")
    own_index = lax.axis_index("blk")
    pairs = n_blk // 2
    degree_dev = legendre.shape[2] // n_blk
    own_pair, own_side = own_index // 2, own_index % 2
    swap = [(i, i + 1 - 2 * (i % 2)) for i in range(n_blk)]

    def terms_for(target):
        table = lax.dynamic_slice_in_dim(legendre, target * degree_dev, degree_dev, 2)
        return jnp.einsum("pml,fpcm->lfcm", table, spectrum, preferred_element_type=jnp.float32)

    def pair_sum(step):
        base = (own_pair + step) % pairs * 2
        given = terms_for(base + 1 - own_side).astype(jnp.bfloat16)
        taken = lax.ppermute(given, "blk", swap)
        return terms_for(base + own_side) + taken.astype(jnp.float32)

    steps = sorted(range(1, pairs), key=lambda step: abs(2 * step - pairs))
    arrived = []
    for step in steps:
        shift = [(i, (i + 2 * step) % n_blk) for i in range(n_blk)]
        arrived.append(lax.ppermute(pair_sum(step).astype(jnp.bfloat16), "blk", shift))
    total = pair_sum(0)
    for piece in arrived:
        total = total + piece.astype(jnp.float32)
    return total


def body(field, ocean_mask, plan, legendre):
    lon_local = field.shape[2]
    slot_dev = legendre.shape[0]
    masked = field * ocean_mask.astype(jnp.float32)[None]
    packed = pack_cycles(masked, plan, slot_dev)
    first = lax.axis_index("order") * lon_local
    terms = transform(packed, twiddle(first, lon_local))
    spectrum = lax.psum_scatter(terms, "order", scatter_dimension=3, tiled=True).astype(
        jnp.bfloat16
    )
    coefficients = degree_sums(legendre, spectrum)
    return coefficients


def solution(mesh):
    placed = (P(None, "blk", "order"), P("blk", "order"), P(), P("blk", "order", None))
    return jax.shard_map(
        body, mesh=mesh, in_specs=placed, out_specs=P("blk", None, None, "order"), check_vma=False
    )
```
